32 devices in a mesh: dp: 16 (over z, y, core), sp: 2 (over x).
Axes of the slice: x: 2, y: 2, z: 4, core: 2. Of those that a mesh axis runs over, the one named last changes fastest.
Arguments:
- hidden: bfloat16 [16, 4, 128, 3584], P('dp', None, 'sp'), may hold values from -6 to 6
- segment_ids: int32 [16, 4, 128], P('dp'), may hold values from -1 to 15, as said below
- w_query: bfloat16 [3584, 3584], P(None, 'sp'), may hold values from -0.10022297 to 0.10022297
- key_matrix: bfloat16 [3584, 512], P(None, 'sp'), may hold values from -0.10022297 to 0.10022297
- value_matrix: bfloat16 [3584, 512], P(None, 'sp'), may hold values from -0.10022297 to 0.10022297
Outputs:
- mixed: bfloat16 [16, 512, 3584], P('dp', 'sp')
The draws below stay inside these ranges and needn't reach their ends.
Inputs may be any that keep to these rules, and one draw needn't show every extreme that they name: `segment_ids`: in each outbox the live slots come first; over them the ids start at 0 and never fall, by steps of 0 or 1; empty slots hold -1. Every group has an outbox whose 128 slots are all live.
All inputs are finite; a program needn't handle non-finite values.
Results may differ from the reference program's by a relative error of at most 0.0087.
Values may be sent and summed in bfloat16 or wider, within the bound.
A program may use at most 64 MiB of HBM per device.

```python
import math
import jax
import jax.numpy as jnp
from jax import lax

MODEL_WIDTH = 3584
QUERY_HEADS = 28
KEY_VALUE_HEADS = 4
HEAD_SIZE = 128
J = 4
B = 128
NSEG = 16
NG = 16
GROUP_SLOTS = 512


def drawn_parts(key):
    key_dir = jax.random.fold_in(key, 21)
    single_key_head = jax.random.fold_in(key, 22)
    direction = jnp.clip(jax.random.normal(key_dir, (MODEL_WIDTH,), jnp.float32), -4.0, 4.0)
    direction = direction / jnp.sqrt(jnp.sum(direction * direction))
    mask_pattern = jnp.clip(jax.random.normal(single_key_head, (KEY_VALUE_HEADS, HEAD_SIZE), jnp.float32), -4.0, 4.0)
    return (direction, mask_pattern)


def draw_w_query(key, part):
    direction, mask_pattern = drawn_parts(key)
    random_noise_key = jax.random.fold_in(key, 31)
    initial_sample = jnp.clip(jax.random.normal(random_noise_key, (MODEL_WIDTH, QUERY_HEADS * HEAD_SIZE), jnp.float32), -5.0, 5.0)
    split_by_head = jnp.repeat(mask_pattern, QUERY_HEADS // KEY_VALUE_HEADS, axis=0).reshape(QUERY_HEADS * HEAD_SIZE)
    weight = initial_sample / math.sqrt(MODEL_WIDTH) + HEAD_SIZE ** (-0.25) * direction[:, None] * split_by_head[None, :]
    bound_value = 6.0 / math.sqrt(MODEL_WIDTH)
    return jnp.clip(weight, -bound_value, bound_value).astype(jnp.bfloat16)


def draw_key_matrix(key, part):
    direction, mask_pattern = drawn_parts(key)
    random_noise_key = jax.random.fold_in(key, 32)
    initial_sample = jnp.clip(jax.random.normal(random_noise_key, (MODEL_WIDTH, KEY_VALUE_HEADS * HEAD_SIZE), jnp.float32), -5.0, 5.0)
    split_by_head = mask_pattern.reshape(KEY_VALUE_HEADS * HEAD_SIZE)
    weight = initial_sample / math.sqrt(MODEL_WIDTH) + HEAD_SIZE ** (-0.25) * direction[:, None] * split_by_head[None, :]
    bound_value = 6.0 / math.sqrt(MODEL_WIDTH)
    return jnp.clip(weight, -bound_value, bound_value).astype(jnp.bfloat16)


def draw_value_matrix(key, part):
    direction = drawn_parts(key)[0]
    random_noise_key = jax.random.fold_in(key, 33)
    initial_sample = jnp.clip(jax.random.normal(random_noise_key, (MODEL_WIDTH, KEY_VALUE_HEADS * HEAD_SIZE), jnp.float32), -5.0, 5.0)
    initial_sample = initial_sample / math.sqrt(MODEL_WIDTH)
    along = jnp.sum(direction[:, None] * initial_sample, axis=0)
    weight = initial_sample - direction[:, None] * along[None, :]
    bound_value = 6.0 / math.sqrt(MODEL_WIDTH)
    return jnp.clip(weight, -bound_value, bound_value).astype(jnp.bfloat16)


def draw_hidden(key, part):
    direction = drawn_parts(key)[0]
    random_noise_key = jax.random.fold_in(key, 41)
    start_key = jax.random.fold_in(key, 42)
    level_key = jax.random.fold_in(key, 43)
    noise_draw = jnp.clip(jax.random.normal(random_noise_key, (NG, J, B, MODEL_WIDTH), jnp.float32), -5.0, 5.0)
    strengths = jnp.array([110.0, 160.0, 220.0, 300.0], jnp.float32)
    run_length = max(B // 8, 2)
    starts = jax.random.randint(start_key, (NG, J), 0, B // 4 - run_length + 1)
    levels = jax.random.randint(level_key, (NG, J), 0, 4)
    picked = (levels[..., None] == jnp.arange(4, dtype=jnp.int32)).astype(jnp.float32)
    amplitude = jnp.sqrt(jnp.sum(picked * strengths, axis=-1))
    slot_index = jnp.arange(B, dtype=jnp.int32)
    inside = (slot_index[None, None, :] >= starts[..., None]) & (slot_index[None, None, :] < starts[..., None] + run_length)
    boost_size = jnp.where(inside, amplitude[..., None], 0.0)
    mixed_rows = noise_draw + boost_size[..., None] * direction
    return jnp.clip(mixed_rows, -6.0, 6.0).astype(jnp.bfloat16)


def draw_segment_ids(key, part):
    key_live = jax.random.fold_in(key, 11)
    key_full = jax.random.fold_in(key, 12)
    key_cuts = jax.random.fold_in(key, 13)
    live_count = jax.random.randint(key_live, (NG, J), B // 4, B + 1)
    full_box = jax.random.randint(key_full, (NG,), 0, J)
    live_count = jnp.where(jnp.arange(J)[None, :] == full_box[:, None], B, live_count)
    index = jnp.arange(B, dtype=jnp.int32)
    cut_marks = (jax.random.randint(key_cuts, (NG, J, B), 0, 12) == 0) & (index[None, None, :] > 0)
    seg_ids = jnp.minimum(jnp.cumsum(cut_marks.astype(jnp.int32), axis=-1), NSEG - 1)
    return jnp.where(index[None, None, :] < live_count[:, :, None], seg_ids, -1).astype(jnp.int32)


def setup_inputs(seed: int = 0) -> dict:
    splits = jax.random.split(jax.random.key(seed), 6)
    hidden = draw_hidden(jax.random.fold_in(splits[5], 71), 0)
    segment_ids = draw_segment_ids(jax.random.fold_in(splits[5], 71), 0)
    w_query = draw_w_query(jax.random.fold_in(splits[5], 71), 0)
    key_matrix = draw_key_matrix(jax.random.fold_in(splits[5], 71), 0)
    value_matrix = draw_value_matrix(jax.random.fold_in(splits[5], 71), 0)
    return dict(hidden=hidden, segment_ids=segment_ids, w_query=w_query, key_matrix=key_matrix, value_matrix=value_matrix)


ROPE_BASE = 1000000.0

def rotate(tensor, where):
    half_width = tensor.shape[-1] // 2
    freq = ROPE_BASE ** (-(jnp.arange(half_width, dtype=jnp.float32) * 2.0 / tensor.shape[-1]))
    angle = where[:, None] * freq[None, :]
    cosine = jnp.cos(angle)[:, None, :]
    sine = jnp.sin(angle)[:, None, :]
    first = tensor[..., :half_width]
    second = tensor[..., half_width:]
    return jnp.concatenate([first * cosine - second * sine, second * cosine + first * sine], axis=-1)

def positions(segments):
    slot_ids = jnp.arange(NSEG, dtype=jnp.int32)
    onehot = (segments[..., :, None] == slot_ids).astype(jnp.int32)
    living = (segments >= 0).astype(jnp.int32)
    below = lax.optimization_barrier(jnp.sum((segments[..., :, None] < slot_ids).astype(jnp.int32) * living[..., :, None], axis=-2))
    first_slot = lax.optimization_barrier(jnp.sum(onehot * below[..., None, :], axis=-1))
    index = jnp.arange(segments.shape[-1], dtype=jnp.int32)
    return (index - first_slot).astype(jnp.float32)

def attend(queries, projected_key_rows, projected_value_rows, labels):
    total_rows = queries.shape[0]
    kv_heads = projected_key_rows.shape[1]
    queries = queries.reshape(total_rows, kv_heads, -1, queries.shape[-1]).astype(jnp.float32)
    scores = jnp.einsum('qcgd,kcd->cgqk', queries, projected_key_rows.astype(jnp.float32)) / jnp.sqrt(jnp.float32(queries.shape[-1]))
    index = jnp.arange(total_rows, dtype=jnp.int32)
    seen = (labels[:, None] == labels[None, :]) & (labels[:, None] >= 0) & (index[None, :] <= index[:, None])
    seen = seen | (index[:, None] == index[None, :])
    scores = jnp.where(seen, scores, -1e+30)
    largest = lax.optimization_barrier(jnp.max(scores, axis=-1, keepdims=True))
    expo = jnp.where(seen, jnp.exp(scores - largest), 0.0)
    denominator = lax.optimization_barrier(jnp.sum(expo, axis=-1, keepdims=True))
    probs = expo.astype(jnp.bfloat16).astype(jnp.float32)
    summed = jnp.einsum('cgqk,kcd->qcgd', probs, projected_value_rows.astype(jnp.float32))
    summed = summed / jnp.transpose(denominator, (2, 0, 1, 3))
    living = (labels >= 0).astype(jnp.float32)
    return (summed.reshape(total_rows, -1) * living[:, None]).astype(jnp.bfloat16)

def reference(hidden, segment_ids, w_query, key_matrix, value_matrix):
    received = jnp.stack([jnp.roll(hidden[:, outbox], outbox, axis=0) for outbox in range(J)], axis=1)
    segments = jnp.stack([jnp.roll(segment_ids[:, outbox], outbox, axis=0) for outbox in range(J)], axis=1)
    where_all = positions(segments)
    box_ids = jnp.arange(J, dtype=jnp.int32)[None, :, None]
    labels = jnp.where(segments >= 0, box_ids * NSEG + segments, -1)

    def one_group(packed):
        slab, where, label_row = packed
        flattened_slots = slab.reshape(GROUP_SLOTS, MODEL_WIDTH)
        where = where.reshape(GROUP_SLOTS)
        queries = jnp.dot(flattened_slots, w_query, preferred_element_type=jnp.float32).reshape(GROUP_SLOTS, QUERY_HEADS, HEAD_SIZE)
        queries = rotate(queries, where).astype(jnp.bfloat16)
        projected_key_rows = jnp.dot(flattened_slots, key_matrix, preferred_element_type=jnp.float32).reshape(GROUP_SLOTS, KEY_VALUE_HEADS, HEAD_SIZE)
        projected_key_rows = rotate(projected_key_rows, where).astype(jnp.bfloat16)
        projected_value_rows = jnp.dot(flattened_slots, value_matrix, preferred_element_type=jnp.float32).astype(jnp.bfloat16).reshape(GROUP_SLOTS, KEY_VALUE_HEADS, HEAD_SIZE)
        return attend(queries, projected_key_rows, projected_value_rows, label_row.reshape(GROUP_SLOTS))
    return lax.map(one_group, (received, where_all, labels))
```

```python
import functools

import jax
import jax.numpy as jnp
from jax import lax
from jax.experimental import pallas as pl
from jax.experimental.pallas import tpu as pltpu
from jax.sharding import PartitionSpec as P

HEAD = 128
ROPE_BASE = 1000000.0
MESH = pl.DeviceIdType.MESH


def kernel(
    n_dp, n_sp, heads_per_kv, chunk,
    hidden, segs, freq, w_query, w_key, w_value, out,
    wbuf, tok, segbuf, qkv, att, cos_ref, sin_ref, bias_ref, live_ref,
    w_sem, own_sem, dp_send, dp_recv, seg_send, seg_recv, x_send, x_recv,
    o_send, o_recv,
):
    boxes = hidden.shape[1]
    slots = segs.shape[2]
    kv_cols, q_cols = w_key.shape[1], w_query.shape[1]
    n_kv = kv_cols // HEAD
    per = chunk // HEAD
    kv_chunks, q_chunks = kv_cols // chunk, q_cols // chunk
    boxes_per = boxes // n_sp
    p = lax.axis_index("dp")
    s = lax.axis_index("sp")

    def order_of(receiver, i):
        if n_sp == 2 and boxes == 4:
            mid = i + 1 - receiver
            last = 1 + 2 * receiver
            if isinstance(i, int):
                if i == 0:
                    return 0
                return last if i == boxes - 1 else mid
            return jnp.where(i == 0, 0, jnp.where(i == boxes - 1, last, mid))
        return i

    def own_order(i):
        return order_of(s, i)

    def forward_order(i):
        return order_of(n_sp - 1 - s, i)

    def weight_copy(c):
        if c < kv_chunks:
            src = w_key.at[:, pl.ds(c * chunk, chunk)]
        elif c < kv_chunks + q_chunks:
            src = w_query.at[:, pl.ds((c - kv_chunks) * chunk, chunk)]
        else:
            src = w_value.at[:, pl.ds((c - kv_chunks - q_chunks) * chunk, chunk)]
        return pltpu.make_async_copy(src, wbuf.at[c], w_sem.at[c])

    def dp_copy(j):
        return pltpu.make_async_remote_copy(
            src_ref=hidden.at[0, j], dst_ref=tok.at[j, s],
            send_sem=dp_send.at[j], recv_sem=dp_recv.at[j],
            device_id=(lax.rem(p + j, n_dp), s), device_id_type=MESH,
        )

    def seg_copy(j):
        return pltpu.make_async_remote_copy(
            src_ref=segs.at[0], dst_ref=segbuf.at[j],
            send_sem=seg_send.at[j], recv_sem=seg_recv.at[j],
            device_id=(lax.rem(p + j, n_dp), s), device_id_type=MESH,
        )

    def x_copy(src, j, k):
        return pltpu.make_async_remote_copy(
            src_ref=src, dst_ref=tok.at[j, s],
            send_sem=x_send.at[j, k - 1], recv_sem=x_recv.at[j, k - 1],
            device_id=(p, lax.rem(s + k, n_sp)), device_id_type=MESH,
        )

    own_copy = pltpu.make_async_copy(hidden.at[0, 0], tok.at[0, s], own_sem)

    barrier = pltpu.get_barrier_semaphore()
    for j in range(1, boxes):
        for q in (lax.rem(p + j, n_dp), lax.rem(p + n_dp - j, n_dp)):
            pl.semaphore_signal(barrier, inc=1, device_id=(q, s), device_id_type=MESH)
    for k in range(1, n_sp):
        pl.semaphore_signal(
            barrier, inc=1, device_id=(p, lax.rem(s + k, n_sp)), device_id_type=MESH
        )
    own_copy.start()
    pl.semaphore_wait(barrier, 2 * (boxes - 1) + n_sp - 1)

    for k in range(1, n_sp):
        x_copy(hidden.at[0, 0], 0, k).start()
    for j in range(1, boxes):
        seg_copy(j).start()
    for i in range(1, boxes):
        dp_copy(forward_order(i)).start()
    total_chunks = 2 * kv_chunks + q_chunks
    for c in range(total_chunks):
        weight_copy(c).start()

    segbuf[0] = segs[0]
    own_copy.wait()
    for j in range(1, boxes):
        seg_copy(j).wait()

    def forward(i):
        j = forward_order(i)
        dp_copy(j).wait_recv()
        for k in range(1, n_sp):
            x_copy(tok.at[j, s], j, k).start()

    def out_slice(j):
        row = pl.multiple_of(lax.rem(j, boxes_per) * slots, slots)
        col = pl.multiple_of(s * q_cols, HEAD)
        return out.at[0, pl.ds(row, slots), pl.ds(col, q_cols)]

    def local_out(i, j):
        return pltpu.make_async_copy(att.at[i], out_slice(j), o_send.at[i])

    def remote_out(i, j):
        owner = j // boxes_per
        k = lax.rem(owner - s + n_sp, n_sp)
        return pltpu.make_async_remote_copy(
            src_ref=att.at[i], dst_ref=out_slice(j),
            send_sem=o_send.at[i], recv_sem=o_recv.at[lax.rem(j, boxes_per), k - 1],
            device_id=(p, owner), device_id_type=MESH,
        )

    def tables(j):
        box = segbuf[j].astype(jnp.float32)
        pick = lax.broadcasted_iota(jnp.int32, box.shape, 0) == j
        row = jnp.sum(jnp.where(pick, box, 0.0), axis=0, keepdims=True)
        r = lax.broadcasted_iota(jnp.int32, (slots, slots), 0)
        c = lax.broadcasted_iota(jnp.int32, (slots, slots), 1)
        row = jnp.broadcast_to(row, (slots, slots))
        col = jnp.sum(jnp.where(r == c, row, 0.0), axis=1, keepdims=True)
        below = jnp.sum(
            jnp.where((row < col) & (row >= 0.0), 1.0, 0.0), axis=1, keepdims=True
        )
        where = r[:, :1].astype(jnp.float32) - below
        angle = where * freq[0:1, :]
        lane = lax.broadcasted_iota(jnp.int32, angle.shape, 1)
        cos_ref[...] = jnp.cos(angle)
        sine = jnp.sin(angle)
        sin_ref[...] = jnp.where(lane < HEAD // 2, -sine, sine)
        seen = ((row == col) & (col >= 0.0) & (c <= r)) | (c == r)
        bias_ref[...] = jnp.where(seen, 0.0, -1e30)
        live_ref[...] = jnp.broadcast_to(
            jnp.where(col >= 0.0, 1.0, 0.0), (slots, HEAD)
        )

    def step(i, carry):
        j = own_order(i)
        tables(j)

        @pl.when(i == 0)
        def _():
            forward(1)

        @pl.when(i == 1)
        def _():
            for later in range(2, boxes):
                forward(later)

        for k in range(1, n_sp):
            source = lax.rem(s + n_sp - k, n_sp)
            pltpu.make_async_remote_copy(
                src_ref=tok.at[j, source], dst_ref=tok.at[j, source],
                send_sem=x_send.at[j, k - 1], recv_sem=x_recv.at[j, k - 1],
                device_id=(p, lax.rem(s + k, n_sp)), device_id_type=MESH,
            ).wait_recv()

        def project(c):
            @pl.when(i == 0)
            def _():
                pltpu.make_async_copy(wbuf.at[c], wbuf.at[c], w_sem.at[c]).wait()

            x = tok[j].reshape(slots, tok.shape[3])
            return jnp.dot(x, wbuf[c], preferred_element_type=jnp.float32)

        def rotated(c, carry):
            prod = project(c)
            for h in range(per):
                t = prod[:, h * HEAD : (h + 1) * HEAD]
                turned = pltpu.roll(t, HEAD // 2, 1)
                qkv[c * per + h] = (t * cos_ref[...] + turned * sin_ref[...]).astype(
                    jnp.bfloat16
                )
            return carry

        lax.fori_loop(0, kv_chunks + q_chunks, rotated, 0)
        for c in range(kv_chunks + q_chunks, total_chunks):
            prod = project(c)
            for h in range(per):
                qkv[c * per + h] = prod[:, h * HEAD : (h + 1) * HEAD].astype(jnp.bfloat16)

        scale = 1.0 / (HEAD ** 0.5)
        bias = bias_ref[...]
        live = live_ref[...]
        v_base = n_kv + n_kv * heads_per_kv
        for g in range(n_kv):
            keys = qkv[g]
            values = qkv[v_base + g]
            for h in range(heads_per_kv):
                head = g * heads_per_kv + h
                scores = lax.dot_general(
                    qkv[n_kv + head], keys, (((1,), (1,)), ((), ())),
                    preferred_element_type=jnp.float32,
                )
                scores = scores * scale + bias
                top = jnp.max(scores, axis=1, keepdims=True)
                e = jnp.exp(scores - top)
                total = jnp.sum(e, axis=1, keepdims=True)
                mixed = jnp.dot(
                    e.astype(jnp.bfloat16), values, preferred_element_type=jnp.float32
                )
                att[i, :, head * HEAD : (head + 1) * HEAD] = (
                    mixed / total * live
                ).astype(jnp.bfloat16)

        @pl.when(j // boxes_per == s)
        def _():
            local_out(i, j).start()

        @pl.when(j // boxes_per != s)
        def _():
            remote_out(i, j).start()

        return carry

    lax.fori_loop(0, boxes, step, 0)

    for j in range(1, boxes):
        dp_copy(j).wait_send()
    for j in range(boxes):
        for k in range(1, n_sp):
            x_copy(tok.at[j, s], j, k).wait_send()
    for i in range(boxes):
        j = own_order(i)

        @pl.when(j // boxes_per == s)
        def _():
            local_out(i, j).wait()

        @pl.when(j // boxes_per != s)
        def _():
            remote_out(i, j).wait_send()

    for b in range(boxes_per):
        for k in range(1, n_sp):
            source = lax.rem(s + n_sp - k, n_sp)
            dst = out.at[
                0, pl.ds(b * slots, slots),
                pl.ds(pl.multiple_of(source * q_cols, HEAD), q_cols),
            ]
            pltpu.make_async_remote_copy(
                src_ref=att.at[0], dst_ref=dst,
                send_sem=o_send.at[0], recv_sem=o_recv.at[b, k - 1],
                device_id=(p, source), device_id_type=MESH,
            ).wait_recv()


def solution(mesh):
    n_dp, n_sp = mesh.shape["dp"], mesh.shape["sp"]

    def local(hidden, segment_ids, w_query, key_matrix, value_matrix):
        boxes, part, width = hidden.shape[1:]
        slots = segment_ids.shape[2]
        q_cols, kv_cols = w_query.shape[1], key_matrix.shape[1]
        chunk = 2 * HEAD if kv_cols % (2 * HEAD) == 0 and q_cols % (2 * HEAD) == 0 else HEAD
        chunks = (q_cols + 2 * kv_cols) // chunk
        heads = (q_cols + 2 * kv_cols) // HEAD
        half = jnp.arange(HEAD // 2, dtype=jnp.float32)
        freq = ROPE_BASE ** (-(half * 2.0 / HEAD))
        freq = jnp.broadcast_to(jnp.concatenate([freq, freq])[None, :], (8, HEAD))
        vmem = pl.BlockSpec(memory_space=pltpu.VMEM)
        hbm = pl.BlockSpec(memory_space=pl.ANY)
        dma = pltpu.SemaphoreType.DMA
        return pl.pallas_call(
            functools.partial(kernel, n_dp, n_sp, q_cols // kv_cols, chunk),
            out_shape=jax.ShapeDtypeStruct(
                (1, boxes * slots // n_sp, q_cols * n_sp), jnp.bfloat16
            ),
            in_specs=[hbm, vmem, vmem, hbm, hbm, hbm],
            out_specs=hbm,
            scratch_shapes=[
                pltpu.VMEM((chunks, width, chunk), jnp.bfloat16),
                pltpu.VMEM((boxes, n_sp, part, width), jnp.bfloat16),
                pltpu.VMEM((boxes, boxes, slots), jnp.int32),
                pltpu.VMEM((heads, slots, HEAD), jnp.bfloat16),
                pltpu.VMEM((boxes, slots, q_cols), jnp.bfloat16),
                pltpu.VMEM((slots, HEAD), jnp.float32),
                pltpu.VMEM((slots, HEAD), jnp.float32),
                pltpu.VMEM((slots, slots), jnp.float32),
                pltpu.VMEM((slots, HEAD), jnp.float32),
                dma((chunks,)),
                dma,
                dma((boxes,)),
                dma((boxes,)),
                dma((boxes,)),
                dma((boxes,)),
                dma((boxes, n_sp - 1)),
                dma((boxes, n_sp - 1)),
                dma((boxes,)),
                dma((boxes // n_sp, n_sp - 1)),
            ],
            compiler_params=pltpu.CompilerParams(
                collective_id=0, has_side_effects=True, vmem_limit_bytes=60 * 1024 * 1024
            ),
            name="rebalanced_attention",
        )(hidden, segment_ids, freq, w_query, key_matrix, value_matrix)

    placed = (
        P("dp", None, "sp", None),
        P("dp", None, None),
        P(None, "sp"),
        P(None, "sp"),
        P(None, "sp"),
    )
    return jax.shard_map(
        local, mesh=mesh, in_specs=placed, out_specs=P("dp", "sp", None), check_vma=False
    )
```

```python
import functools

import jax
import jax.numpy as jnp
import numpy as np
from jax import lax
from jax.experimental import pallas as pl
from jax.experimental.pallas import tpu as pltpu
from jax.sharding import PartitionSpec as P

HEAD = 128
ROPE_BASE = 1000000.0
PIECES = 2
MESH = pl.DeviceIdType.MESH


def kernel(
    n_dp, n_sp, heads_per_kv, chunk,
    hidden, segs, freq, w_query, w_key, w_value, out,
    wbuf, tok, segbuf, qkv, att, cos_ref, sin_ref, bias_ref, live_ref,
    w_sem, own_sem, dp_send, dp_recv, seg_send, seg_recv, x_send, x_recv,
    o_send, o_recv,
):
    boxes = hidden.shape[1]
    slots = segs.shape[2]
    kv_cols, q_cols = w_key.shape[1], w_query.shape[1]
    n_kv = kv_cols // HEAD
    per = chunk // HEAD
    kv_chunks, q_chunks = kv_cols // chunk, q_cols // chunk
    boxes_per = boxes // n_sp
    p = lax.axis_index("dp")
    s = lax.axis_index("sp")

    def order_of(receiver, i):
        if n_sp == 2 and boxes == 4:
            mid = i + 1 - receiver
            last = 1 + 2 * receiver
            if isinstance(i, int):
                if i == 0:
                    return 0
                return last if i == boxes - 1 else mid
            return jnp.where(i == 0, 0, jnp.where(i == boxes - 1, last, mid))
        return i

    def own_order(i):
        return order_of(s, i)

    def forward_order(i):
        return order_of(n_sp - 1 - s, i)

    def weight_copy(c):
        if c < kv_chunks:
            src = w_key.at[:, pl.ds(c * chunk, chunk)]
        elif c < kv_chunks + q_chunks:
            src = w_query.at[:, pl.ds((c - kv_chunks) * chunk, chunk)]
        else:
            src = w_value.at[:, pl.ds((c - kv_chunks - q_chunks) * chunk, chunk)]
        return pltpu.make_async_copy(src, wbuf.at[c], w_sem.at[c])

    rows = hidden.shape[2] // PIECES

    def piece(ref, h):
        return ref.at[pl.ds(h * rows, rows)]

    def dp_copy(j, h):
        return pltpu.make_async_remote_copy(
            src_ref=piece(hidden.at[0, j], h), dst_ref=piece(tok.at[j, s], h),
            send_sem=dp_send.at[j, h], recv_sem=dp_recv.at[j, h],
            device_id=(lax.rem(p + j, n_dp), s), device_id_type=MESH,
        )

    def seg_copy(j):
        return pltpu.make_async_remote_copy(
            src_ref=segs.at[0], dst_ref=segbuf.at[j],
            send_sem=seg_send.at[j], recv_sem=seg_recv.at[j],
            device_id=(lax.rem(p + j, n_dp), s), device_id_type=MESH,
        )

    def x_copy(src, j, k, h):
        return pltpu.make_async_remote_copy(
            src_ref=piece(src, h), dst_ref=piece(tok.at[j, s], h),
            send_sem=x_send.at[j, k - 1, h], recv_sem=x_recv.at[j, k - 1, h],
            device_id=(p, lax.rem(s + k, n_sp)), device_id_type=MESH,
        )

    own_copy = pltpu.make_async_copy(hidden.at[0, 0], tok.at[0, s], own_sem)

    barrier = pltpu.get_barrier_semaphore()
    for j in range(1, boxes):
        for q in (lax.rem(p + j, n_dp), lax.rem(p + n_dp - j, n_dp)):
            pl.semaphore_signal(barrier, inc=1, device_id=(q, s), device_id_type=MESH)
    for k in range(1, n_sp):
        pl.semaphore_signal(
            barrier, inc=1, device_id=(p, lax.rem(s + k, n_sp)), device_id_type=MESH
        )
    own_copy.start()
    pl.semaphore_wait(barrier, 2 * (boxes - 1) + n_sp - 1)

    for j in range(1, boxes):
        seg_copy(j).start()
    for h in range(PIECES):
        for k in range(1, n_sp):
            x_copy(hidden.at[0, 0], 0, k, h).start()
    for i in range(1, boxes):
        for h in range(PIECES):
            dp_copy(forward_order(i), h).start()
    total_chunks = 2 * kv_chunks + q_chunks
    for c in range(total_chunks):
        weight_copy(c).start()

    segbuf[0] = segs[0]
    own_copy.wait()
    for j in range(1, boxes):
        seg_copy(j).wait()

    def forward(i):
        j = forward_order(i)
        for h in range(PIECES):
            dp_copy(j, h).wait_recv()
            for k in range(1, n_sp):
                x_copy(tok.at[j, s], j, k, h).start()

    def out_slice(j):
        row = pl.multiple_of(lax.rem(j, boxes_per) * slots, slots)
        col = pl.multiple_of(s * q_cols, HEAD)
        return out.at[0, pl.ds(row, slots), pl.ds(col, q_cols)]

    def local_out(i, j):
        return pltpu.make_async_copy(att.at[i], out_slice(j), o_send.at[i])

    def remote_out(i, j):
        owner = j // boxes_per
        k = lax.rem(owner - s + n_sp, n_sp)
        return pltpu.make_async_remote_copy(
            src_ref=att.at[i], dst_ref=out_slice(j),
            send_sem=o_send.at[i], recv_sem=o_recv.at[lax.rem(j, boxes_per), k - 1],
            device_id=(p, owner), device_id_type=MESH,
        )

    def tables(j):
        box = segbuf[j].astype(jnp.float32)
        pick = lax.broadcasted_iota(jnp.int32, box.shape, 0) == j
        row = jnp.sum(jnp.where(pick, box, 0.0), axis=0, keepdims=True)
        r = lax.broadcasted_iota(jnp.int32, (slots, slots), 0)
        c = lax.broadcasted_iota(jnp.int32, (slots, slots), 1)
        row = jnp.broadcast_to(row, (slots, slots))
        col = jnp.sum(jnp.where(r == c, row, 0.0), axis=1, keepdims=True)
        below = jnp.sum(
            jnp.where((row < col) & (row >= 0.0), 1.0, 0.0), axis=1, keepdims=True
        )
        where = r[:, :1].astype(jnp.float32) - below
        angle = where * freq[0:1, :]
        lane = lax.broadcasted_iota(jnp.int32, angle.shape, 1)
        cos_ref[...] = jnp.cos(angle)
        sine = jnp.sin(angle)
        sin_ref[...] = jnp.where(lane < HEAD // 2, -sine, sine)
        seen = ((row == col) & (col >= 0.0) & (c <= r)) | (c == r)
        bias_ref[...] = jnp.where(seen, 0.0, -1e30)
        live_ref[...] = jnp.broadcast_to(
            jnp.where(col >= 0.0, 1.0, 0.0), (slots, HEAD)
        )

    def step(i, carry):
        j = own_order(i)
        tables(j)

        @pl.when(i == 0)
        def _():
            forward(1)

        @pl.when(i == 1)
        def _():
            for later in range(2, boxes):
                forward(later)

        for k in range(1, n_sp):
            source = lax.rem(s + n_sp - k, n_sp)
            for h in range(PIECES):
                half = piece(tok.at[j, source], h)
                pltpu.make_async_remote_copy(
                    src_ref=half, dst_ref=half,
                    send_sem=x_send.at[j, k - 1, h], recv_sem=x_recv.at[j, k - 1, h],
                    device_id=(p, source), device_id_type=MESH,
                ).wait_recv()

        def project(c):
            @pl.when(i == 0)
            def _():
                pltpu.make_async_copy(wbuf.at[c], wbuf.at[c], w_sem.at[c]).wait()

            x = tok[j].reshape(slots, tok.shape[3])
            return jnp.dot(x, wbuf[c], preferred_element_type=jnp.float32)

        def rotated(c, carry):
            prod = project(c)
            for h in range(per):
                t = prod[:, h * HEAD : (h + 1) * HEAD]
                turned = pltpu.roll(t, HEAD // 2, 1)
                qkv[c * per + h] = (t * cos_ref[...] + turned * sin_ref[...]).astype(
                    jnp.bfloat16
                )
            return carry

        lax.fori_loop(0, kv_chunks + q_chunks, rotated, 0)
        for c in range(kv_chunks + q_chunks, total_chunks):
            prod = project(c)
            for h in range(per):
                qkv[c * per + h] = prod[:, h * HEAD : (h + 1) * HEAD].astype(jnp.bfloat16)

        scale = 1.0 / (HEAD ** 0.5)
        bias = bias_ref[...]
        live = live_ref[...]
        v_base = n_kv + n_kv * heads_per_kv
        for g in range(n_kv):
            keys = qkv[g]
            values = qkv[v_base + g]
            for h in range(heads_per_kv):
                head = g * heads_per_kv + h
                scores = lax.dot_general(
                    qkv[n_kv + head], keys, (((1,), (1,)), ((), ())),
                    preferred_element_type=jnp.float32,
                )
                scores = scores * scale + bias
                top = jnp.max(scores, axis=1, keepdims=True)
                e = jnp.exp(scores - top)
                total = jnp.sum(e, axis=1, keepdims=True)
                mixed = jnp.dot(
                    e.astype(jnp.bfloat16), values, preferred_element_type=jnp.float32
                )
                att[i, :, head * HEAD : (head + 1) * HEAD] = (
                    mixed / total * live
                ).astype(jnp.bfloat16)

        @pl.when(j // boxes_per == s)
        def _():
            local_out(i, j).start()

        @pl.when(j // boxes_per != s)
        def _():
            remote_out(i, j).start()

        return carry

    lax.fori_loop(0, boxes, step, 0)

    for h in range(PIECES):
        for j in range(1, boxes):
            dp_copy(j, h).wait_send()
        for j in range(boxes):
            for k in range(1, n_sp):
                x_copy(tok.at[j, s], j, k, h).wait_send()
    for i in range(boxes):
        j = own_order(i)

        @pl.when(j // boxes_per == s)
        def _():
            local_out(i, j).wait()

        @pl.when(j // boxes_per != s)
        def _():
            remote_out(i, j).wait_send()

    for b in range(boxes_per):
        for k in range(1, n_sp):
            source = lax.rem(s + n_sp - k, n_sp)
            dst = out.at[
                0, pl.ds(b * slots, slots),
                pl.ds(pl.multiple_of(source * q_cols, HEAD), q_cols),
            ]
            pltpu.make_async_remote_copy(
                src_ref=att.at[0], dst_ref=dst,
                send_sem=o_send.at[0], recv_sem=o_recv.at[b, k - 1],
                device_id=(p, source), device_id_type=MESH,
            ).wait_recv()


def solution(mesh):
    n_dp, n_sp = mesh.shape["dp"], mesh.shape["sp"]

    def local(hidden, segment_ids, w_query, key_matrix, value_matrix):
        boxes, part, width = hidden.shape[1:]
        slots = segment_ids.shape[2]
        q_cols, kv_cols = w_query.shape[1], key_matrix.shape[1]
        chunk = 2 * HEAD if kv_cols % (2 * HEAD) == 0 and q_cols % (2 * HEAD) == 0 else HEAD
        chunks = (q_cols + 2 * kv_cols) // chunk
        heads = (q_cols + 2 * kv_cols) // HEAD
        half = np.arange(HEAD // 2, dtype=np.float64)
        freq = ROPE_BASE ** (-(half * 2.0 / HEAD))
        freq = jnp.asarray(np.tile(freq, (8, 2)).astype(np.float32))
        vmem = pl.BlockSpec(memory_space=pltpu.VMEM)
        hbm = pl.BlockSpec(memory_space=pl.ANY)
        dma = pltpu.SemaphoreType.DMA
        return pl.pallas_call(
            functools.partial(kernel, n_dp, n_sp, q_cols // kv_cols, chunk),
            out_shape=pltpu.VMEM((1, boxes * slots // n_sp, q_cols * n_sp), jnp.bfloat16),
            in_specs=[hbm, vmem, vmem, hbm, hbm, hbm],
            out_specs=vmem,
            scratch_shapes=[
                pltpu.VMEM((chunks, width, chunk), jnp.bfloat16),
                pltpu.VMEM((boxes, n_sp, part, width), jnp.bfloat16),
                pltpu.VMEM((boxes, boxes, slots), jnp.int32),
                pltpu.VMEM((heads, slots, HEAD), jnp.bfloat16),
                pltpu.VMEM((boxes, slots, q_cols), jnp.bfloat16),
                pltpu.VMEM((slots, HEAD), jnp.float32),
                pltpu.VMEM((slots, HEAD), jnp.float32),
                pltpu.VMEM((slots, slots), jnp.float32),
                pltpu.VMEM((slots, HEAD), jnp.float32),
                dma((chunks,)),
                dma,
                dma((boxes, PIECES)),
                dma((boxes, PIECES)),
                dma((boxes,)),
                dma((boxes,)),
                dma((boxes, n_sp - 1, PIECES)),
                dma((boxes, n_sp - 1, PIECES)),
                dma((boxes,)),
                dma((boxes // n_sp, n_sp - 1)),
            ],
            compiler_params=pltpu.CompilerParams(
                collective_id=0, has_side_effects=True, vmem_limit_bytes=60 * 1024 * 1024
            ),
            name="rebalanced_attention",
        )(hidden, segment_ids, freq, w_query, key_matrix, value_matrix)

    placed = (
        P("dp", None, "sp", None),
        P("dp", None, None),
        P(None, "sp"),
        P(None, "sp"),
        P(None, "sp"),
    )
    return jax.shard_map(
        local, mesh=mesh, in_specs=placed, out_specs=P("dp", "sp", None), check_vma=False
    )
```

```python
import functools

import jax
import jax.numpy as jnp
import numpy as np
from jax import lax
from jax.experimental import pallas as pl
from jax.experimental.pallas import tpu as pltpu
from jax.sharding import PartitionSpec as P

HEAD = 128
ROPE_BASE = 1000000.0
PIECES = 2
MESH = pl.DeviceIdType.MESH


def kernel(
    n_dp, n_sp, heads_per_kv, chunk,
    hidden, segs, freq_hbm, w_query, w_key, w_value, out,
    wbuf, tok, segbuf, qkv, att, cos_ref, sin_ref, bias_ref, live_ref, freq,
    w_sem, own_sem, own_seg_sem, freq_sem, dp_send, dp_recv, seg_send, seg_recv, x_send, x_recv,
    o_send, o_recv,
):
    boxes = hidden.shape[1]
    slots = segs.shape[2]
    kv_cols, q_cols = w_key.shape[1], w_query.shape[1]
    n_kv = kv_cols // HEAD
    per = chunk // HEAD
    kv_chunks, q_chunks = kv_cols // chunk, q_cols // chunk
    boxes_per = boxes // n_sp
    p = lax.axis_index("dp")
    s = lax.axis_index("sp")

    def order_of(receiver, i):
        if n_sp == 2 and boxes == 4:
            mid = i + 1 - receiver
            last = 1 + 2 * receiver
            if isinstance(i, int):
                if i == 0:
                    return 0
                return last if i == boxes - 1 else mid
            return jnp.where(i == 0, 0, jnp.where(i == boxes - 1, last, mid))
        return i

    def own_order(i):
        return order_of(s, i)

    def forward_order(i):
        return order_of(n_sp - 1 - s, i)

    def weight_copy(c):
        if c < kv_chunks:
            src = w_key.at[:, pl.ds(c * chunk, chunk)]
        elif c < kv_chunks + q_chunks:
            src = w_query.at[:, pl.ds((c - kv_chunks) * chunk, chunk)]
        else:
            src = w_value.at[:, pl.ds((c - kv_chunks - q_chunks) * chunk, chunk)]
        return pltpu.make_async_copy(src, wbuf.at[c], w_sem.at[c])

    rows = hidden.shape[2] // PIECES

    def piece(ref, h):
        return ref.at[pl.ds(h * rows, rows)]

    def dp_copy(j, h):
        return pltpu.make_async_remote_copy(
            src_ref=piece(hidden.at[0, j], h), dst_ref=piece(tok.at[j, s], h),
            send_sem=dp_send.at[j, h], recv_sem=dp_recv.at[j, h],
            device_id=(lax.rem(p + j, n_dp), s), device_id_type=MESH,
        )

    def seg_copy(j):
        return pltpu.make_async_remote_copy(
            src_ref=segs.at[0], dst_ref=segbuf.at[j],
            send_sem=seg_send.at[j], recv_sem=seg_recv.at[j],
            device_id=(lax.rem(p + j, n_dp), s), device_id_type=MESH,
        )

    def x_copy(src, j, k, h):
        return pltpu.make_async_remote_copy(
            src_ref=piece(src, h), dst_ref=piece(tok.at[j, s], h),
            send_sem=x_send.at[j, k - 1, h], recv_sem=x_recv.at[j, k - 1, h],
            device_id=(p, lax.rem(s + k, n_sp)), device_id_type=MESH,
        )

    own_copy = pltpu.make_async_copy(hidden.at[0, 0], tok.at[0, s], own_sem)

    barrier = pltpu.get_barrier_semaphore()
    for j in range(1, boxes):
        pl.semaphore_signal(
            barrier, inc=1, device_id=(lax.rem(p + n_dp - j, n_dp), s), device_id_type=MESH
        )
    for k in range(1, n_sp):
        pl.semaphore_signal(
            barrier, inc=1, device_id=(p, lax.rem(s + k, n_sp)), device_id_type=MESH
        )
    own_copy.start()
    own_segs = pltpu.make_async_copy(segs.at[0], segbuf.at[0], own_seg_sem)
    freq_copy = pltpu.make_async_copy(freq_hbm, freq, freq_sem)
    own_segs.start()
    freq_copy.start()
    pl.semaphore_wait(barrier, boxes - 1 + n_sp - 1)

    for j in range(1, boxes):
        seg_copy(j).start()
    for h in range(PIECES):
        for k in range(1, n_sp):
            x_copy(hidden.at[0, 0], 0, k, h).start()
    for i in range(1, boxes):
        for h in range(PIECES):
            dp_copy(forward_order(i), h).start()
    total_chunks = 2 * kv_chunks + q_chunks
    for c in range(total_chunks):
        weight_copy(c).start()

    freq_copy.wait()
    own_segs.wait()
    own_copy.wait()
    for j in range(1, boxes):
        seg_copy(j).wait()

    def forward(i):
        j = forward_order(i)
        for h in range(PIECES):
            dp_copy(j, h).wait_recv()
            for k in range(1, n_sp):
                x_copy(tok.at[j, s], j, k, h).start()

    def out_slice(j):
        row = pl.multiple_of(lax.rem(j, boxes_per) * slots, slots)
        col = pl.multiple_of(s * q_cols, HEAD)
        return out.at[0, pl.ds(row, slots), pl.ds(col, q_cols)]

    def local_out(i, j):
        return pltpu.make_async_copy(att.at[i], out_slice(j), o_send.at[i])

    def remote_out(i, j):
        owner = j // boxes_per
        k = lax.rem(owner - s + n_sp, n_sp)
        return pltpu.make_async_remote_copy(
            src_ref=att.at[i], dst_ref=out_slice(j),
            send_sem=o_send.at[i], recv_sem=o_recv.at[lax.rem(j, boxes_per), k - 1],
            device_id=(p, owner), device_id_type=MESH,
        )

    def tables(j):
        box = segbuf[j].astype(jnp.float32)
        pick = lax.broadcasted_iota(jnp.int32, box.shape, 0) == j
        row = jnp.sum(jnp.where(pick, box, 0.0), axis=0, keepdims=True)
        r = lax.broadcasted_iota(jnp.int32, (slots, slots), 0)
        c = lax.broadcasted_iota(jnp.int32, (slots, slots), 1)
        row = jnp.broadcast_to(row, (slots, slots))
        col = jnp.sum(jnp.where(r == c, row, 0.0), axis=1, keepdims=True)
        below = jnp.sum(
            jnp.where((row < col) & (row >= 0.0), 1.0, 0.0), axis=1, keepdims=True
        )
        where = r[:, :1].astype(jnp.float32) - below
        angle = where * freq[0:1, :]
        lane = lax.broadcasted_iota(jnp.int32, angle.shape, 1)
        cos_ref[...] = jnp.cos(angle)
        sine = jnp.sin(angle)
        sin_ref[...] = jnp.where(lane < HEAD // 2, -sine, sine)
        seen = ((row == col) & (col >= 0.0) & (c <= r)) | (c == r)
        bias_ref[...] = jnp.where(seen, 0.0, -1e30)
        live_ref[...] = jnp.broadcast_to(
            jnp.where(col >= 0.0, 1.0, 0.0), (slots, HEAD)
        )

    def step(i, carry):
        j = own_order(i)
        tables(j)

        @pl.when(i == 0)
        def _():
            forward(1)

        @pl.when(i == 1)
        def _():
            for later in range(2, boxes):
                forward(later)

        for k in range(1, n_sp):
            source = lax.rem(s + n_sp - k, n_sp)
            for h in range(PIECES):
                half = piece(tok.at[j, source], h)
                pltpu.make_async_remote_copy(
                    src_ref=half, dst_ref=half,
                    send_sem=x_send.at[j, k - 1, h], recv_sem=x_recv.at[j, k - 1, h],
                    device_id=(p, source), device_id_type=MESH,
                ).wait_recv()

        def project(c):
            @pl.when(i == 0)
            def _():
                pltpu.make_async_copy(wbuf.at[c], wbuf.at[c], w_sem.at[c]).wait()

            x = tok[j].reshape(slots, tok.shape[3])
            return jnp.dot(x, wbuf[c], preferred_element_type=jnp.float32)

        def rotated(c, carry):
            prod = project(c)
            for h in range(per):
                t = prod[:, h * HEAD : (h + 1) * HEAD]
                turned = pltpu.roll(t, HEAD // 2, 1)
                qkv[c * per + h] = (t * cos_ref[...] + turned * sin_ref[...]).astype(
                    jnp.bfloat16
                )
            return carry

        lax.fori_loop(0, kv_chunks + q_chunks, rotated, 0)
        for c in range(kv_chunks + q_chunks, total_chunks):
            prod = project(c)
            for h in range(per):
                qkv[c * per + h] = prod[:, h * HEAD : (h + 1) * HEAD].astype(jnp.bfloat16)

        scale = 1.0 / (HEAD ** 0.5)
        bias = bias_ref[...]
        live = live_ref[...]
        v_base = n_kv + n_kv * heads_per_kv
        for g in range(n_kv):
            keys = qkv[g]
            values = qkv[v_base + g]
            for h in range(heads_per_kv):
                head = g * heads_per_kv + h
                scores = lax.dot_general(
                    qkv[n_kv + head], keys, (((1,), (1,)), ((), ())),
                    preferred_element_type=jnp.float32,
                )
                scores = scores * scale + bias
                top = jnp.max(scores, axis=1, keepdims=True)
                e = jnp.exp(scores - top)
                total = jnp.sum(e, axis=1, keepdims=True)
                mixed = jnp.dot(
                    e.astype(jnp.bfloat16), values, preferred_element_type=jnp.float32
                )
                att[i, :, head * HEAD : (head + 1) * HEAD] = (
                    mixed / total * live
                ).astype(jnp.bfloat16)

        @pl.when(j // boxes_per == s)
        def _():
            local_out(i, j).start()

        @pl.when(j // boxes_per != s)
        def _():
            remote_out(i, j).start()

        return carry

    lax.fori_loop(0, boxes, step, 0)

    for h in range(PIECES):
        for j in range(1, boxes):
            dp_copy(j, h).wait_send()
        for j in range(boxes):
            for k in range(1, n_sp):
                x_copy(tok.at[j, s], j, k, h).wait_send()
    for i in range(boxes):
        j = own_order(i)

        @pl.when(j // boxes_per == s)
        def _():
            local_out(i, j).wait()

        @pl.when(j // boxes_per != s)
        def _():
            remote_out(i, j).wait_send()

    for b in range(boxes_per):
        for k in range(1, n_sp):
            source = lax.rem(s + n_sp - k, n_sp)
            dst = out.at[
                0, pl.ds(b * slots, slots),
                pl.ds(pl.multiple_of(source * q_cols, HEAD), q_cols),
            ]
            pltpu.make_async_remote_copy(
                src_ref=att.at[0], dst_ref=dst,
                send_sem=o_send.at[0], recv_sem=o_recv.at[b, k - 1],
                device_id=(p, source), device_id_type=MESH,
            ).wait_recv()


def solution(mesh):
    n_dp, n_sp = mesh.shape["dp"], mesh.shape["sp"]

    def local(hidden, segment_ids, w_query, key_matrix, value_matrix):
        boxes, part, width = hidden.shape[1:]
        slots = segment_ids.shape[2]
        q_cols, kv_cols = w_query.shape[1], key_matrix.shape[1]
        chunk = 2 * HEAD if kv_cols % (2 * HEAD) == 0 and q_cols % (2 * HEAD) == 0 else HEAD
        chunks = (q_cols + 2 * kv_cols) // chunk
        heads = (q_cols + 2 * kv_cols) // HEAD
        half = np.arange(HEAD // 2, dtype=np.float64)
        freq = ROPE_BASE ** (-(half * 2.0 / HEAD))
        freq = jnp.asarray(np.tile(freq, (8, 2)).astype(np.float32))
        vmem = pl.BlockSpec(memory_space=pltpu.VMEM)
        hbm = pl.BlockSpec(memory_space=pl.ANY)
        dma = pltpu.SemaphoreType.DMA
        return pl.pallas_call(
            functools.partial(kernel, n_dp, n_sp, q_cols // kv_cols, chunk),
            out_shape=pltpu.VMEM((1, boxes * slots // n_sp, q_cols * n_sp), jnp.bfloat16),
            in_specs=[hbm] * 6,
            out_specs=vmem,
            scratch_shapes=[
                pltpu.VMEM((chunks, width, chunk), jnp.bfloat16),
                pltpu.VMEM((boxes, n_sp, part, width), jnp.bfloat16),
                pltpu.VMEM((boxes, boxes, slots), jnp.int32),
                pltpu.VMEM((heads, slots, HEAD), jnp.bfloat16),
                pltpu.VMEM((boxes, slots, q_cols), jnp.bfloat16),
                pltpu.VMEM((slots, HEAD), jnp.float32),
                pltpu.VMEM((slots, HEAD), jnp.float32),
                pltpu.VMEM((slots, slots), jnp.float32),
                pltpu.VMEM((slots, HEAD), jnp.float32),
                pltpu.VMEM((8, HEAD), jnp.float32),
                dma((chunks,)),
                dma,
                dma,
                dma,
                dma((boxes, PIECES)),
                dma((boxes, PIECES)),
                dma((boxes,)),
                dma((boxes,)),
                dma((boxes, n_sp - 1, PIECES)),
                dma((boxes, n_sp - 1, PIECES)),
                dma((boxes,)),
                dma((boxes // n_sp, n_sp - 1)),
            ],
            compiler_params=pltpu.CompilerParams(
                collective_id=0, has_side_effects=True, vmem_limit_bytes=60 * 1024 * 1024
            ),
            name="rebalanced_attention",
        )(hidden, segment_ids, freq, w_query, key_matrix, value_matrix)

    placed = (
        P("dp", None, "sp", None),
        P("dp", None, None),
        P(None, "sp"),
        P(None, "sp"),
        P(None, "sp"),
    )
    return jax.shard_map(
        local, mesh=mesh, in_specs=placed, out_specs=P("dp", "sp", None), check_vma=False
    )
```
